32 devices in a mesh: dp: 32 (over z, y, x, core).
Axes of the slice: x: 2, y: 2, z: 4, core: 2. Of those that a mesh axis runs over, the one named last changes fastest.
Arguments:
- grads: float32 [32, 1048576], P('dp')
- master: float32 [1048576], P('dp'), may hold values from -0.75 to 0.75
- m_old: float32 [32, 65536], P('dp'), may hold values from -6 to 6
- v_old: float32 [32, 65536], P('dp'), may hold values from 0.25 to 4
- old_bounds: int32 [33], replicated, may hold values from 0 to 1048576, as said below
Outputs:
- master_new: float32 [1048576], P('dp')
- m_new: float32 [1048576], P('dp')
- v_new: float32 [1048576], P('dp')
- params_full: bfloat16 [1048576], replicated
The draws below stay inside these ranges and needn't reach their ends.
Inputs may be any that keep to these rules, and one draw needn't show every extreme that they name: old_bounds[0] = 0, the last entry is 1048576, entries never fall, and old_bounds[i] - i * 32768 lies between -16384 and 16384 for every i. Row k of m_old and v_old holds its span in its first old_bounds[k+1] - old_bounds[k] slots; later slots are unused. Some span has exactly 65536 entries in every draw.
All inputs are finite; a program needn't handle non-finite values.
Results may differ from the reference program's by a relative error of at most 0.0049.
Values may be sent and summed in bfloat16 or wider, within the bound.
A program may use at most 128 MiB of HBM per device.

```python
import math
import jax
import jax.numpy as jnp
from jax import lax

ND = 32768
FLAT = 1048576
CAP = 65536
N_DP = 32


def draw_grads(key, part):
    first = jax.random.fold_in(jax.random.fold_in(key, 21), 0)
    fourth = jax.random.fold_in(jax.random.fold_in(key, 21), 3)
    fifth = jax.random.fold_in(jax.random.fold_in(key, 21), 4)
    positions = jnp.arange(FLAT, dtype=jnp.float32)
    ramp = 1.0 + 2.0 * positions / FLAT
    block_level = jnp.exp(jax.random.uniform(fourth, (N_DP, 1), jnp.float32, -0.8, 0.8))
    level = (block_level * jnp.ones((1, ND), jnp.float32)).reshape(FLAT)
    overall = jnp.exp(jax.random.uniform(fifth, (), jnp.float32, -1.0, 1.0))
    values = jax.random.normal(first, (N_DP, FLAT), jnp.float32) * (ramp * level * overall)
    return values.astype(jnp.float32)


def draw_old_bounds(key, part):
    first, second = jax.random.split(jax.random.fold_in(key, 11))
    margin = ND // 2
    drift = jax.random.randint(first, (N_DP + 1,), -margin, margin + 1)
    chosen = jax.random.randint(second, (), 1, N_DP - 1)
    index_all = jnp.arange(N_DP + 1, dtype=jnp.int32)
    drift = jnp.where(index_all == chosen, -margin, drift)
    drift = jnp.where(index_all == chosen + 1, margin, drift)
    drift = jnp.where((index_all == 0) | (index_all == N_DP), 0, drift)
    return (index_all * ND + drift).astype(jnp.int32)


def block_scale(stream_key, extent, cuts, low, largest):
    loudness, own = 1.0, jax.random.fold_in(stream_key, 6)
    for position, shards_of in cuts:
        heights = jnp.exp(jax.random.uniform(jax.random.fold_in(own, position), (shards_of,), jnp.float32, low / len(cuts), largest / len(cuts)))
        loudness = loudness * jnp.repeat(heights, extent[position] // shards_of).reshape([-1 if axis == position else 1 for axis in range(len(extent))])
    return loudness


def centred(stream_key, dims, deviation, bound, shards=(), kind=jnp.bfloat16):
    drawn = jax.random.normal(stream_key, dims, jnp.float32) * deviation
    if len(shards) > 0:
        drawn = block_scale(stream_key, dims, shards, -0.22, 0.18) * drawn
    return jnp.clip(drawn, min=-bound, max=bound).astype(kind)


def setup_inputs(seed: int = 0) -> dict:
    key_list = jax.random.split(jax.random.key(seed), 6)
    return {
        "grads": draw_grads(jax.random.fold_in(key_list[5], 71), 0),
        "master": centred(key_list[1], (FLAT,), 0.05, 0.75, ((0, 32),), jnp.float32),
        "m_old": centred(key_list[2], (N_DP, CAP), 1.0, 6.0, ((0, 32),), jnp.float32),
        "v_old": jnp.clip(jnp.exp(math.log(4.0) - 2.7725887 * jax.random.uniform(key_list[3], (N_DP, CAP), jnp.float32) ** block_scale(key_list[3], (N_DP, CAP), ((0, 32),), -0.2, 0.2)), 0.25, 4.0),
        "old_bounds": draw_old_bounds(jax.random.fold_in(key_list[5], 71), 0),
    }


def reference(grads, master, m_old, v_old, old_bounds):
    gradient = lax.optimization_barrier(jnp.sum(grads, axis=0))
    positions = jnp.arange(FLAT, dtype=jnp.int32)
    owner = (jnp.searchsorted(old_bounds, positions, side='right') - 1).astype(jnp.int32)
    slot = (positions - old_bounds[owner]).astype(jnp.int32)
    m_prev = m_old[owner, slot]
    v_prev = v_old[owner, slot]
    total = jnp.sum(gradient * gradient)
    clip = jnp.minimum(1.0, jnp.sqrt(jnp.float32(FLAT)) / (jnp.sqrt(total) + 1e-06))
    clipped = clip * gradient
    m_new = 0.5 * m_prev + 0.5 * clipped
    v_new = 0.95 * v_prev + 0.05 * clipped * clipped
    direction = m_new / (1.0 - 0.5 ** 20) / (jnp.sqrt(v_new / (1.0 - 0.95 ** 20)) + 1e-08)
    master_new = master - 0.05 * (direction + 0.1 * master)
    return (master_new, m_new, v_new, master_new.astype(jnp.bfloat16))
```

```python
import functools

import jax
import jax.numpy as jnp
from jax import lax
from jax.experimental import pallas as pl
from jax.experimental.pallas import tpu as pltpu
from jax.sharding import PartitionSpec as P

MESH = pl.DeviceIdType.MESH
LANES = 128
F32 = jnp.float32
BF16 = jnp.bfloat16


def grid_of(count):
    sizes, chips, turn = [1, 1, 1], count // 2, 0
    while chips > 1:
        sizes[turn % 3] *= 2
        chips //= 2
        turn += 1
    return tuple(sizes)


def kernel(
    dims, grads, master, m_old, v_old, bounds,
    master_out, m_out, v_out, full,
    own_a, own_b, mate_a, mate_b,
    send_a1, send_b1, recv_a1, recv_b1,
    send_a2, send_b2, recv_a2, recv_b2, keep_a, keep_b,
    send_z, recv_z, gradient,
    spans, here, edge_out, edge_in, prev, weights, norm_out, norm_in,
    load_sem, own_sem_a, own_sem_b,
    mate_ss_a, mate_rs_a, mate_ss_b, mate_rs_b,
    ss_a1, rs_a1, ss_b1, rs_b1, ss_a2, rs_a2, ss_b2, rs_b2, ss_z, rs_z,
    edge_ss, edge_rs, norm_ss, norm_rs,
    gz_ss, gz_rs, gx_ss, gx_rs, gy_ss, gy_rs, gxy_ss, gxy_rs, gyx_ss, gyx_rs,
    d_ss, d_rs, dx_ss, dx_rs, dy_ss, dy_rs, dxy_ss, dxy_rs, dyx_ss, dyx_rs,
):
    Z, Y, X = dims
    count = Z * Y * X * 2
    rows = master.shape[0]
    half = rows // 2
    me = lax.axis_index("dp")
    core = me % 2
    x = (me // 2) % X
    y = (me // (2 * X)) % Y
    z = me // (2 * X * Y)

    def device(zz, yy, xx, cc):
        return ((zz * Y + yy) * X + xx) * 2 + cc

    mate = device(z, y, x, 1 - core)

    def at(coord, step, size):
        return (coord + step) % size

    sends = []

    def send(src, dst, ss, rs, target):
        copy = pltpu.make_async_remote_copy(
            src_ref=src, dst_ref=dst, send_sem=ss, recv_sem=rs,
            device_id=(target,), device_id_type=MESH)
        copy.start()
        sends.append(copy)

    def arrived(dst, ss, rs):
        pltpu.make_async_remote_copy(
            src_ref=dst, dst_ref=dst, send_sem=ss, recv_sem=rs,
            device_id=(mate,), device_id_type=MESH).wait_recv()

    barrier = pltpu.get_barrier_semaphore()

    @pl.loop(1, count)
    def _(step):
        pl.semaphore_signal(barrier, inc=1, device_id=((me + step) % count,), device_id_type=MESH)

    pad = rows + 8
    load_m = pltpu.make_async_copy(m_old, spans.at[0, pl.ds(pad, 2 * rows)], load_sem.at[0])
    load_v = pltpu.make_async_copy(v_old, spans.at[1, pl.ds(pad, 2 * rows)], load_sem.at[1])
    load_w = pltpu.make_async_copy(master, weights, load_sem.at[2])
    load_m.start()
    load_v.start()
    order = [s for s in sorted(range(1, Z), key=lambda s: abs(s - Z / 2))] + [0]
    first, second = slice(0, half), slice(half, rows)
    loads_a, loads_b = {}, {}
    for s in order:
        for o in list(range(1, X)) + [0]:
            loads_a[o, s] = pltpu.make_async_copy(
                grads.at[at(z, s, Z), :, at(x, o, X), core, pl.ds(0, half)],
                own_a.at[o, s], own_sem_a.at[o, s])
            loads_a[o, s].start()
        for o in list(range(1, Y)) + [0]:
            loads_b[o, s] = pltpu.make_async_copy(
                grads.at[at(z, s, Z), at(y, o, Y), :, core, pl.ds(half, half)],
                own_b.at[o, s], own_sem_b.at[o, s])
            loads_b[o, s].start()
    load_w.start()

    here_bound = bounds[me] - me * (rows * LANES)
    next_bound = bounds[me + 1] - me * (rows * LANES)
    shift = jnp.clip(here_bound + half * LANES, 0, rows * LANES)
    lift, turn = shift // LANES, shift % LANES
    spans[:, pl.ds(0, pad)] = jnp.zeros((2, pad, LANES), F32)
    load_m.wait()
    load_v.wait()
    tile = 32
    lane = lax.broadcasted_iota(jnp.int32, (tile, LANES), 1)

    def aligned(which, row):
        base = pad + row - lift
        now = pltpu.roll(spans[which, pl.ds(base, tile)], turn, 1)
        before = pltpu.roll(spans[which, pl.ds(base - 1, tile)], turn, 1)
        return jnp.where(lane >= turn, now, before)

    for which in range(2):
        @pl.loop(0, half // tile)
        def _(i, which=which):
            row = pl.multiple_of(i * tile, tile)
            edge_out[0, which, pl.ds(row, tile)] = aligned(which, row).astype(BF16)
            edge_out[1, which, pl.ds(row, tile)] = aligned(which, row + 3 * half).astype(BF16)
            here[which, pl.ds(row, tile)] = aligned(which, row + half)
            here[which, pl.ds(row + half, tile)] = aligned(which, row + 2 * half)

    pl.semaphore_wait(barrier, count - 1)

    for s in order:
        for o in list(range(1, X)) + [0]:
            send(grads.at[at(z, s, Z), :, at(x, o, X), 1 - core, pl.ds(0, half)],
                 mate_a.at[o, s], mate_ss_a.at[o, s], mate_rs_a.at[o, s], mate)
        for o in list(range(1, Y)) + [0]:
            send(grads.at[at(z, s, Z), at(y, o, Y), :, 1 - core, pl.ds(half, half)],
                 mate_b.at[o, s], mate_ss_b.at[o, s], mate_rs_b.at[o, s], mate)

    def chip_ready_a(o, s):
        loads_a[o, s].wait()
        arrived(mate_a.at[o, s], mate_ss_a.at[o, s], mate_rs_a.at[o, s])

    def chip_ready_b(o, s):
        loads_b[o, s].wait()
        arrived(mate_b.at[o, s], mate_ss_b.at[o, s], mate_rs_b.at[o, s])

    def exchange_one(s):
        for o in range(1, X):
            chip_ready_a(o, s)
            for j in range(Y):
                send_a1[o - 1, s, j] = (own_a[o, s, j] + mate_a[o, s, j]).astype(BF16)
            send(send_a1.at[o - 1, s], recv_a1.at[o - 1, s], ss_a1.at[o - 1, s], rs_a1.at[o - 1, s],
                 device(z, y, at(x, o, X), core))
        for o in range(1, Y):
            chip_ready_b(o, s)
            for j in range(X):
                send_b1[o - 1, s, j] = (own_b[o, s, j] + mate_b[o, s, j]).astype(BF16)
            send(send_b1.at[o - 1, s], recv_b1.at[o - 1, s], ss_b1.at[o - 1, s], rs_b1.at[o - 1, s],
                 device(z, at(y, o, Y), x, core))

    def exchange_two(s):
        chip_ready_a(0, s)
        for o in range(1, X):
            arrived(recv_a1.at[o - 1, s], ss_a1.at[o - 1, s], rs_a1.at[o - 1, s])

        def sum_a(j):
            value = own_a[0, s, j] + mate_a[0, s, j]
            for o in range(1, X):
                value = value + recv_a1[o - 1, s, j].astype(F32)
            return value

        for o in range(1, Y):
            send_a2[o - 1, s] = sum_a(at(y, o, Y)).astype(BF16)
            send(send_a2.at[o - 1, s], recv_a2.at[o - 1, s], ss_a2.at[o - 1, s], rs_a2.at[o - 1, s],
                 device(z, at(y, o, Y), x, core))
        keep_a[s] = sum_a(y)
        chip_ready_b(0, s)
        for o in range(1, Y):
            arrived(recv_b1.at[o - 1, s], ss_b1.at[o - 1, s], rs_b1.at[o - 1, s])

        def sum_b(j):
            value = own_b[0, s, j] + mate_b[0, s, j]
            for o in range(1, Y):
                value = value + recv_b1[o - 1, s, j].astype(F32)
            return value

        for o in range(1, X):
            send_b2[o - 1, s] = sum_b(at(x, o, X)).astype(BF16)
            send(send_b2.at[o - 1, s], recv_b2.at[o - 1, s], ss_b2.at[o - 1, s], rs_b2.at[o - 1, s],
                 device(z, y, at(x, o, X), core))
        keep_b[s] = sum_b(x)

    def exchange_three(s):
        for o in range(1, Y):
            arrived(recv_a2.at[o - 1, s], ss_a2.at[o - 1, s], rs_a2.at[o - 1, s])
        value_a = keep_a[s]
        for o in range(1, Y):
            value_a = value_a + recv_a2[o - 1, s].astype(F32)
        for o in range(1, X):
            arrived(recv_b2.at[o - 1, s], ss_b2.at[o - 1, s], rs_b2.at[o - 1, s])
        value_b = keep_b[s]
        for o in range(1, X):
            value_b = value_b + recv_b2[o - 1, s].astype(F32)
        if s == 0:
            gradient[pl.ds(0, half)] = value_a
            gradient[pl.ds(half, half)] = value_b
        else:
            send_z[s - 1, pl.ds(0, half)] = value_a.astype(BF16)
            send_z[s - 1, pl.ds(half, half)] = value_b.astype(BF16)
            send(send_z.at[s - 1], recv_z.at[s - 1], ss_z.at[s - 1], rs_z.at[s - 1],
                 device(at(z, s, Z), y, x, core))

    for s in order:
        exchange_one(s)
    send(edge_out.at[0], edge_in.at[0], edge_ss.at[0], edge_rs.at[0], (me + count - 1) % count)
    send(edge_out.at[1], edge_in.at[1], edge_ss.at[1], edge_rs.at[1], (me + 1) % count)
    for i in range(Z + 1):
        if i < Z:
            exchange_two(order[i])
        if i > 0:
            exchange_three(order[i - 1])
    for s in order[:-1]:
        arrived(recv_z.at[s - 1], ss_z.at[s - 1], rs_z.at[s - 1])

    squares = jnp.zeros((8, LANES), F32)
    for i in range(rows // tile):
        part = gradient[pl.ds(i * tile, tile)]
        for s in order[:-1]:
            part = part + recv_z[s - 1, pl.ds(i * tile, tile)].astype(F32)
        gradient[pl.ds(i * tile, tile)] = part
        squares = squares + jnp.sum((part * part).reshape(tile // 8, 8, LANES), axis=0)
    mine = jnp.sum(squares, axis=0, keepdims=True)
    norm_out[...] = mine
    norm_in[me] = mine

    @pl.loop(1, count)
    def _(step):
        pltpu.make_async_remote_copy(
            src_ref=norm_out, dst_ref=norm_in.at[me], send_sem=norm_ss.at[step], recv_sem=norm_rs.at[me],
            device_id=((me + step) % count,), device_id_type=MESH).start()

    for e in range(2):
        arrived(edge_in.at[e], edge_ss.at[e], edge_rs.at[e])
    place = lax.broadcasted_iota(jnp.int32, (tile, LANES), 0) * LANES + lane

    @pl.loop(0, half // tile)
    def _(i):
        row = pl.multiple_of(i * tile, tile)
        low = row * LANES + place
        high = low + half * LANES
        for which in range(2):
            prev[which, pl.ds(row, tile)] = jnp.where(
                low < here_bound, edge_in[1, which, pl.ds(row, tile)].astype(F32),
                here[which, pl.ds(row, tile)])
            prev[which, pl.ds(row + half, tile)] = jnp.where(
                high >= next_bound, edge_in[0, which, pl.ds(row, tile)].astype(F32),
                here[which, pl.ds(row + half, tile)])

    load_w.wait()

    @pl.loop(1, count)
    def _(step):
        other = (me + step) % count
        pltpu.make_async_remote_copy(
            src_ref=norm_out, dst_ref=norm_in.at[other], send_sem=norm_ss.at[step], recv_sem=norm_rs.at[other],
            device_id=(other,), device_id_type=MESH).wait()

    total = jnp.sum(jnp.sum(norm_in[...], axis=0), axis=1, keepdims=True)
    size = jnp.float32(count * rows * LANES)
    clip = jnp.minimum(1.0, jnp.sqrt(size) / (jnp.sqrt(total) + 1e-06))

    for i in range(rows // tile):
        part = pl.ds(i * tile, tile)
        clipped = clip * gradient[part]
        m_new = 0.5 * prev[0, part] + 0.5 * clipped
        v_new = 0.95 * prev[1, part] + 0.05 * clipped * clipped
        direction = m_new / (1.0 - 0.5**20) / (jnp.sqrt(v_new / (1.0 - 0.95**20)) + 1e-08)
        weight = weights[part]
        weight = weight - 0.05 * (direction + 0.1 * weight)
        full[z, y, x, core, part] = weight.astype(BF16)
        master_out[part] = weight
        m_out[part] = m_new
        v_out[part] = v_new

    lower, upper = pl.ds(0, half), pl.ds(half, half)

    def spread(s):
        zz = at(z, Z - s, Z)
        block = full.at[zz, y, x, core]
        if s > 0:
            arrived(block, gz_ss.at[s - 1], gz_rs.at[s - 1])
        for o in range(1, X):
            send(block, block, gx_ss.at[o - 1, s], gx_rs.at[o - 1, s], device(z, y, at(x, o, X), core))
        for o in range(1, Y):
            send(block, block, gy_ss.at[o - 1, s], gy_rs.at[o - 1, s], device(z, at(y, o, Y), x, core))
        send(block, block, d_ss.at[s], d_rs.at[s], mate)

    def turn_corner(s):
        zz = at(z, Z - s, Z)
        for o in range(1, X):
            block = full.at[zz, y, at(x, X - o, X), core]
            arrived(block, gx_ss.at[o - 1, s], gx_rs.at[o - 1, s])
            for p in range(1, Y):
                send(block.at[lower], block.at[lower], gxy_ss.at[o - 1, p - 1, s], gxy_rs.at[o - 1, p - 1, s],
                     device(z, at(y, p, Y), x, core))
            send(block, block, dx_ss.at[o - 1, s], dx_rs.at[o - 1, s], mate)
        for p in range(1, Y):
            block = full.at[zz, at(y, Y - p, Y), x, core]
            arrived(block, gy_ss.at[p - 1, s], gy_rs.at[p - 1, s])
            for o in range(1, X):
                send(block.at[upper], block.at[upper], gyx_ss.at[o - 1, p - 1, s], gyx_rs.at[o - 1, p - 1, s],
                     device(z, y, at(x, o, X), core))
            send(block, block, dy_ss.at[p - 1, s], dy_rs.at[p - 1, s], mate)

    def finish(s):
        zz = at(z, Z - s, Z)
        for o in range(1, X):
            for p in range(1, Y):
                block = full.at[zz, at(y, Y - p, Y), at(x, X - o, X), core]
                index = (o - 1, p - 1, s)
                arrived(block.at[lower], gxy_ss.at[index], gxy_rs.at[index])
                send(block.at[lower], block.at[lower], dxy_ss.at[index], dxy_rs.at[index], mate)
                arrived(block.at[upper], gyx_ss.at[index], gyx_rs.at[index])
                send(block.at[upper], block.at[upper], dyx_ss.at[index], dyx_rs.at[index], mate)

    mine = full.at[z, y, x, core]
    for s in order[:-1]:
        send(mine, mine, gz_ss.at[s - 1], gz_rs.at[s - 1], device(at(z, s, Z), y, x, core))
    ring = [0] + sorted(range(1, Z), key=lambda s: -abs(s - Z / 2))
    for i in range(Z + 2):
        if i < Z:
            spread(ring[i])
        if 0 <= i - 1 < Z:
            turn_corner(ring[i - 1])
        if 0 <= i - 2 < Z:
            finish(ring[i - 2])
    for s in range(Z):
        zz = at(z, Z - s, Z)
        arrived(full.at[zz, y, x, 1 - core], d_ss.at[s], d_rs.at[s])
        for o in range(1, X):
            arrived(full.at[zz, y, at(x, X - o, X), 1 - core], dx_ss.at[o - 1, s], dx_rs.at[o - 1, s])
        for p in range(1, Y):
            arrived(full.at[zz, at(y, Y - p, Y), x, 1 - core], dy_ss.at[p - 1, s], dy_rs.at[p - 1, s])
            for o in range(1, X):
                block = full.at[zz, at(y, Y - p, Y), at(x, X - o, X), 1 - core]
                index = (o - 1, p - 1, s)
                arrived(block.at[lower], dxy_ss.at[index], dxy_rs.at[index])
                arrived(block.at[upper], dyx_ss.at[index], dyx_rs.at[index])
    for copy in sends:
        copy.wait_send()


def local(dims, grads, master, m_old, v_old, old_bounds):
    Z, Y, X = dims
    count = Z * Y * X * 2
    width = master.shape[0]
    rows = width // LANES
    half = rows // 2
    dma = pltpu.SemaphoreType.DMA
    two = lambda *shape: [dma(shape), dma(shape)]
    vmem = pltpu.VMEM
    anywhere = pl.BlockSpec(memory_space=pl.ANY)
    inside = pl.BlockSpec(memory_space=pltpu.VMEM)
    scratch = [
        vmem((X, Z, Y, half, LANES), F32), vmem((Y, Z, X, half, LANES), F32),
        vmem((X, Z, Y, half, LANES), F32), vmem((Y, Z, X, half, LANES), F32),
        vmem((X - 1, Z, Y, half, LANES), BF16), vmem((Y - 1, Z, X, half, LANES), BF16),
        vmem((X - 1, Z, Y, half, LANES), BF16), vmem((Y - 1, Z, X, half, LANES), BF16),
        vmem((Y - 1, Z, half, LANES), BF16), vmem((X - 1, Z, half, LANES), BF16),
        vmem((Y - 1, Z, half, LANES), BF16), vmem((X - 1, Z, half, LANES), BF16),
        vmem((Z, half, LANES), F32), vmem((Z, half, LANES), F32),
        vmem((Z - 1, rows, LANES), BF16), vmem((Z - 1, rows, LANES), BF16),
        vmem((rows, LANES), F32),
        vmem((2, 3 * rows + 8, LANES), F32), vmem((2, rows, LANES), F32),
        vmem((2, 2, half, LANES), BF16), vmem((2, 2, half, LANES), BF16),
        vmem((2, rows, LANES), F32), vmem((rows, LANES), F32),
        vmem((1, LANES), F32), vmem((count, 1, LANES), F32),
        dma((3,)), dma((X, Z)), dma((Y, Z)),
        *two(X, Z), *two(Y, Z),
        *two(X - 1, Z), *two(Y - 1, Z), *two(Y - 1, Z), *two(X - 1, Z), *two(Z - 1),
        *two(2), *two(count),
        *two(Z - 1), *two(X - 1, Z), *two(Y - 1, Z), *two(X - 1, Y - 1, Z), *two(X - 1, Y - 1, Z),
        *two(Z), *two(X - 1, Z), *two(Y - 1, Z), *two(X - 1, Y - 1, Z), *two(X - 1, Y - 1, Z),
    ]
    flat = jax.ShapeDtypeStruct((rows, LANES), F32)
    master_new, m_new, v_new, full = pl.pallas_call(
        functools.partial(kernel, dims),
        out_shape=(flat, flat, flat, jax.ShapeDtypeStruct((Z, Y, X, 2, rows, LANES), BF16)),
        in_specs=[anywhere] * 4 + [pl.BlockSpec(memory_space=pltpu.SMEM)],
        out_specs=(inside,) * 4,
        scratch_shapes=scratch,
        compiler_params=pltpu.CompilerParams(
            collective_id=0, has_side_effects=True, vmem_limit_bytes=60 * 1024 * 1024),
    )(
        grads.reshape(Z, Y, X, 2, rows, LANES),
        master.reshape(rows, LANES),
        m_old.reshape(2 * rows, LANES),
        v_old.reshape(2 * rows, LANES),
        old_bounds,
    )
    return (master_new.reshape(width), m_new.reshape(width), v_new.reshape(width), full.reshape(count * width))


def solution(mesh):
    dims = grid_of(mesh.shape["dp"])
    return jax.shard_map(
        functools.partial(local, dims),
        mesh=mesh,
        in_specs=(P("dp", None), P("dp"), P("dp", None), P("dp", None), P()),
        out_specs=(P("dp"), P("dp"), P("dp"), P()),
        check_vma=False,
    )
```

```python
import functools

import jax
import jax.numpy as jnp
from jax import lax
from jax.experimental import pallas as pl
from jax.experimental.pallas import tpu as pltpu
from jax.sharding import PartitionSpec as P

MESH = pl.DeviceIdType.MESH
LANES = 128
VMEM_BYTES = 127 * 512 * 1024
F32 = jnp.float32
BF16 = jnp.bfloat16


def grid_of(count):
    sizes, chips, turn = [1, 1, 1], count // 2, 0
    while chips > 1:
        sizes[turn % 3] *= 2
        chips //= 2
        turn += 1
    return tuple(sizes)


def kernel(
    dims, grads, master, m_old, v_old, bounds,
    master_out, m_out, v_out, full,
    own_a, own_b, mate_a, mate_b,
    send_a1, send_b1, recv_a1, recv_b1,
    send_a2, send_b2, recv_a2, recv_b2, keep_a, keep_b,
    send_z, recv_z, gradient,
    spans, here, edge_out, edge_in, prev, weights, norm_out, norm_in,
    load_sem, own_sem_a, own_sem_b,
    mate_ss_a, mate_rs_a, mate_ss_b, mate_rs_b,
    ss_a1, rs_a1, ss_b1, rs_b1, ss_a2, rs_a2, ss_b2, rs_b2, ss_z, rs_z,
    edge_ss, edge_rs, norm_ss, norm_rs,
    gz_ss, gz_rs, gx_ss, gx_rs, gy_ss, gy_rs, gxy_ss, gxy_rs, gyx_ss, gyx_rs,
    d_ss, d_rs, dx_ss, dx_rs, dy_ss, dy_rs, dxy_ss, dxy_rs, dyx_ss, dyx_rs,
):
    Z, Y, X = dims
    count = Z * Y * X * 2
    rows = master.shape[0]
    half = rows // 2
    me = lax.axis_index("dp")
    core = me % 2
    x = (me // 2) % X
    y = (me // (2 * X)) % Y
    z = me // (2 * X * Y)

    def device(zz, yy, xx, cc):
        return ((zz * Y + yy) * X + xx) * 2 + cc

    mate = device(z, y, x, 1 - core)

    def at(coord, step, size):
        return (coord + step) % size

    sends = []

    def send(src, dst, ss, rs, target):
        copy = pltpu.make_async_remote_copy(
            src_ref=src, dst_ref=dst, send_sem=ss, recv_sem=rs,
            device_id=(target,), device_id_type=MESH)
        copy.start()
        sends.append(copy)

    def arrived(dst, ss, rs):
        pltpu.make_async_remote_copy(
            src_ref=dst, dst_ref=dst, send_sem=ss, recv_sem=rs,
            device_id=(mate,), device_id_type=MESH).wait_recv()

    barrier = pltpu.get_barrier_semaphore()

    @pl.loop(1, count)
    def _(step):
        pl.semaphore_signal(barrier, inc=1, device_id=((me + step) % count,), device_id_type=MESH)

    pad = rows + 8
    load_m = pltpu.make_async_copy(m_old, spans.at[0, pl.ds(pad, 2 * rows)], load_sem.at[0])
    load_v = pltpu.make_async_copy(v_old, spans.at[1, pl.ds(pad, 2 * rows)], load_sem.at[1])
    load_w = pltpu.make_async_copy(master, weights, load_sem.at[2])
    load_m.start()
    load_v.start()
    order = [s for s in sorted(range(1, Z), key=lambda s: abs(s - Z / 2))] + [0]
    first, second = slice(0, half), slice(half, rows)
    loads_a, loads_b = {}, {}
    for s in order:
        for o in list(range(1, X)) + [0]:
            loads_a[o, s] = pltpu.make_async_copy(
                grads.at[at(z, s, Z), :, at(x, o, X), core, pl.ds(0, half)],
                own_a.at[o, s], own_sem_a.at[o, s])
            loads_a[o, s].start()
        for o in list(range(1, Y)) + [0]:
            loads_b[o, s] = pltpu.make_async_copy(
                grads.at[at(z, s, Z), at(y, o, Y), :, core, pl.ds(half, half)],
                own_b.at[o, s], own_sem_b.at[o, s])
            loads_b[o, s].start()
    load_w.start()

    here_bound = bounds[me] - me * (rows * LANES)
    next_bound = bounds[me + 1] - me * (rows * LANES)
    shift = jnp.clip(here_bound + half * LANES, 0, rows * LANES)
    lift, turn = shift // LANES, shift % LANES
    spans[:, pl.ds(0, pad)] = jnp.zeros((2, pad, LANES), F32)
    load_m.wait()
    load_v.wait()
    tile = 32
    lane = lax.broadcasted_iota(jnp.int32, (tile, LANES), 1)

    def aligned(which, row):
        base = pad + row - lift
        now = pltpu.roll(spans[which, pl.ds(base, tile)], turn, 1)
        before = pltpu.roll(spans[which, pl.ds(base - 1, tile)], turn, 1)
        return jnp.where(lane >= turn, now, before)

    for which in range(2):
        @pl.loop(0, half // tile)
        def _(i, which=which):
            row = pl.multiple_of(i * tile, tile)
            edge_out[0, which, pl.ds(row, tile)] = aligned(which, row).astype(BF16)
            edge_out[1, which, pl.ds(row, tile)] = aligned(which, row + 3 * half).astype(BF16)
            here[which, pl.ds(row, tile)] = aligned(which, row + half)
            here[which, pl.ds(row + half, tile)] = aligned(which, row + 2 * half)

    pl.semaphore_wait(barrier, count - 1)

    for s in order:
        for o in list(range(1, X)) + [0]:
            send(grads.at[at(z, s, Z), :, at(x, o, X), 1 - core, pl.ds(0, half)],
                 mate_a.at[o, s], mate_ss_a.at[o, s], mate_rs_a.at[o, s], mate)
        for o in list(range(1, Y)) + [0]:
            send(grads.at[at(z, s, Z), at(y, o, Y), :, 1 - core, pl.ds(half, half)],
                 mate_b.at[o, s], mate_ss_b.at[o, s], mate_rs_b.at[o, s], mate)

    def chip_ready_a(o, s):
        loads_a[o, s].wait()
        arrived(mate_a.at[o, s], mate_ss_a.at[o, s], mate_rs_a.at[o, s])

    def chip_ready_b(o, s):
        loads_b[o, s].wait()
        arrived(mate_b.at[o, s], mate_ss_b.at[o, s], mate_rs_b.at[o, s])

    def exchange_one(s):
        for o in range(1, X):
            chip_ready_a(o, s)
            for j in range(Y):
                send_a1[o - 1, s, j] = (own_a[o, s, j] + mate_a[o, s, j]).astype(BF16)
            send(send_a1.at[o - 1, s], recv_a1.at[o - 1, s], ss_a1.at[o - 1, s], rs_a1.at[o - 1, s],
                 device(z, y, at(x, o, X), core))
        for o in range(1, Y):
            chip_ready_b(o, s)
            for j in range(X):
                send_b1[o - 1, s, j] = (own_b[o, s, j] + mate_b[o, s, j]).astype(BF16)
            send(send_b1.at[o - 1, s], recv_b1.at[o - 1, s], ss_b1.at[o - 1, s], rs_b1.at[o - 1, s],
                 device(z, at(y, o, Y), x, core))

    def exchange_two(s):
        chip_ready_a(0, s)
        for o in range(1, X):
            arrived(recv_a1.at[o - 1, s], ss_a1.at[o - 1, s], rs_a1.at[o - 1, s])

        def sum_a(j):
            value = own_a[0, s, j] + mate_a[0, s, j]
            for o in range(1, X):
                value = value + recv_a1[o - 1, s, j].astype(F32)
            return value

        for o in range(1, Y):
            send_a2[o - 1, s] = sum_a(at(y, o, Y)).astype(BF16)
            send(send_a2.at[o - 1, s], recv_a2.at[o - 1, s], ss_a2.at[o - 1, s], rs_a2.at[o - 1, s],
                 device(z, at(y, o, Y), x, core))
        keep_a[s] = sum_a(y)
        chip_ready_b(0, s)
        for o in range(1, Y):
            arrived(recv_b1.at[o - 1, s], ss_b1.at[o - 1, s], rs_b1.at[o - 1, s])

        def sum_b(j):
            value = own_b[0, s, j] + mate_b[0, s, j]
            for o in range(1, Y):
                value = value + recv_b1[o - 1, s, j].astype(F32)
            return value

        for o in range(1, X):
            send_b2[o - 1, s] = sum_b(at(x, o, X)).astype(BF16)
            send(send_b2.at[o - 1, s], recv_b2.at[o - 1, s], ss_b2.at[o - 1, s], rs_b2.at[o - 1, s],
                 device(z, y, at(x, o, X), core))
        keep_b[s] = sum_b(x)

    def exchange_three(s):
        for o in range(1, Y):
            arrived(recv_a2.at[o - 1, s], ss_a2.at[o - 1, s], rs_a2.at[o - 1, s])
        value_a = keep_a[s]
        for o in range(1, Y):
            value_a = value_a + recv_a2[o - 1, s].astype(F32)
        for o in range(1, X):
            arrived(recv_b2.at[o - 1, s], ss_b2.at[o - 1, s], rs_b2.at[o - 1, s])
        value_b = keep_b[s]
        for o in range(1, X):
            value_b = value_b + recv_b2[o - 1, s].astype(F32)
        if s == 0:
            gradient[pl.ds(0, half)] = value_a
            gradient[pl.ds(half, half)] = value_b
        else:
            send_z[s - 1, pl.ds(0, half)] = value_a.astype(BF16)
            send_z[s - 1, pl.ds(half, half)] = value_b.astype(BF16)
            send(send_z.at[s - 1], recv_z.at[s - 1], ss_z.at[s - 1], rs_z.at[s - 1],
                 device(at(z, s, Z), y, x, core))

    for s in order:
        exchange_one(s)
    send(edge_out.at[0], edge_in.at[0], edge_ss.at[0], edge_rs.at[0], (me + count - 1) % count)
    send(edge_out.at[1], edge_in.at[1], edge_ss.at[1], edge_rs.at[1], (me + 1) % count)
    for i in range(Z + 1):
        if i < Z:
            exchange_two(order[i])
        if i > 0:
            exchange_three(order[i - 1])
    for s in order[:-1]:
        arrived(recv_z.at[s - 1], ss_z.at[s - 1], rs_z.at[s - 1])

    squares = jnp.zeros((8, LANES), F32)
    for i in range(rows // tile):
        part = gradient[pl.ds(i * tile, tile)]
        for s in order[:-1]:
            part = part + recv_z[s - 1, pl.ds(i * tile, tile)].astype(F32)
        gradient[pl.ds(i * tile, tile)] = part
        squares = squares + jnp.sum((part * part).reshape(tile // 8, 8, LANES), axis=0)
    mine = jnp.sum(squares, axis=0, keepdims=True)
    norm_out[...] = mine
    norm_in[me] = mine

    @pl.loop(1, count)
    def _(step):
        pltpu.make_async_remote_copy(
            src_ref=norm_out, dst_ref=norm_in.at[me], send_sem=norm_ss.at[step], recv_sem=norm_rs.at[me],
            device_id=((me + step) % count,), device_id_type=MESH).start()

    for e in range(2):
        arrived(edge_in.at[e], edge_ss.at[e], edge_rs.at[e])
    place = lax.broadcasted_iota(jnp.int32, (tile, LANES), 0) * LANES + lane

    @pl.loop(0, half // tile)
    def _(i):
        row = pl.multiple_of(i * tile, tile)
        low = row * LANES + place
        high = low + half * LANES
        for which in range(2):
            prev[which, pl.ds(row, tile)] = jnp.where(
                low < here_bound, edge_in[1, which, pl.ds(row, tile)].astype(F32),
                here[which, pl.ds(row, tile)])
            prev[which, pl.ds(row + half, tile)] = jnp.where(
                high >= next_bound, edge_in[0, which, pl.ds(row, tile)].astype(F32),
                here[which, pl.ds(row + half, tile)])

    load_w.wait()

    @pl.loop(1, count)
    def _(step):
        other = (me + step) % count
        pltpu.make_async_remote_copy(
            src_ref=norm_out, dst_ref=norm_in.at[other], send_sem=norm_ss.at[step], recv_sem=norm_rs.at[other],
            device_id=(other,), device_id_type=MESH).wait()

    total = jnp.sum(jnp.sum(norm_in[...], axis=0), axis=1, keepdims=True)
    size = jnp.float32(count * rows * LANES)
    clip = jnp.minimum(1.0, jnp.sqrt(size) / (jnp.sqrt(total) + 1e-06))

    for i in range(rows // tile):
        part = pl.ds(i * tile, tile)
        clipped = clip * gradient[part]
        m_new = 0.5 * prev[0, part] + 0.5 * clipped
        v_new = 0.95 * prev[1, part] + 0.05 * clipped * clipped
        direction = m_new / (1.0 - 0.5**20) / (jnp.sqrt(v_new / (1.0 - 0.95**20)) + 1e-08)
        weight = weights[part]
        weight = weight - 0.05 * (direction + 0.1 * weight)
        full[z, y, x, core, part] = weight.astype(BF16)
        master_out[part] = weight
        m_out[part] = m_new
        v_out[part] = v_new

    lower, upper = pl.ds(0, half), pl.ds(half, half)

    def spread(s):
        zz = at(z, Z - s, Z)
        block = full.at[zz, y, x, core]
        if s > 0:
            arrived(block, gz_ss.at[s - 1], gz_rs.at[s - 1])
        for o in range(1, X):
            send(block, block, gx_ss.at[o - 1, s], gx_rs.at[o - 1, s], device(z, y, at(x, o, X), core))
        for o in range(1, Y):
            send(block, block, gy_ss.at[o - 1, s], gy_rs.at[o - 1, s], device(z, at(y, o, Y), x, core))
        send(block, block, d_ss.at[s], d_rs.at[s], mate)

    def turn_corner(s):
        zz = at(z, Z - s, Z)
        for o in range(1, X):
            block = full.at[zz, y, at(x, X - o, X), core]
            arrived(block, gx_ss.at[o - 1, s], gx_rs.at[o - 1, s])
            for p in range(1, Y):
                send(block.at[lower], block.at[lower], gxy_ss.at[o - 1, p - 1, s], gxy_rs.at[o - 1, p - 1, s],
                     device(z, at(y, p, Y), x, core))
            send(block, block, dx_ss.at[o - 1, s], dx_rs.at[o - 1, s], mate)
        for p in range(1, Y):
            block = full.at[zz, at(y, Y - p, Y), x, core]
            arrived(block, gy_ss.at[p - 1, s], gy_rs.at[p - 1, s])
            for o in range(1, X):
                send(block.at[upper], block.at[upper], gyx_ss.at[o - 1, p - 1, s], gyx_rs.at[o - 1, p - 1, s],
                     device(z, y, at(x, o, X), core))
            send(block, block, dy_ss.at[p - 1, s], dy_rs.at[p - 1, s], mate)

    def finish(s):
        zz = at(z, Z - s, Z)
        for o in range(1, X):
            for p in range(1, Y):
                block = full.at[zz, at(y, Y - p, Y), at(x, X - o, X), core]
                index = (o - 1, p - 1, s)
                arrived(block.at[lower], gxy_ss.at[index], gxy_rs.at[index])
                send(block.at[lower], block.at[lower], dxy_ss.at[index], dxy_rs.at[index], mate)
                arrived(block.at[upper], gyx_ss.at[index], gyx_rs.at[index])
                send(block.at[upper], block.at[upper], dyx_ss.at[index], dyx_rs.at[index], mate)

    mine = full.at[z, y, x, core]
    for s in order[:-1]:
        send(mine, mine, gz_ss.at[s - 1], gz_rs.at[s - 1], device(at(z, s, Z), y, x, core))
    ring = [0] + sorted(range(1, Z), key=lambda s: -abs(s - Z / 2))
    for i in range(Z + 2):
        if i < Z:
            spread(ring[i])
        if 0 <= i - 1 < Z:
            turn_corner(ring[i - 1])
        if 0 <= i - 2 < Z:
            finish(ring[i - 2])
    for s in range(Z):
        zz = at(z, Z - s, Z)
        arrived(full.at[zz, y, x, 1 - core], d_ss.at[s], d_rs.at[s])
        for o in range(1, X):
            arrived(full.at[zz, y, at(x, X - o, X), 1 - core], dx_ss.at[o - 1, s], dx_rs.at[o - 1, s])
        for p in range(1, Y):
            arrived(full.at[zz, at(y, Y - p, Y), x, 1 - core], dy_ss.at[p - 1, s], dy_rs.at[p - 1, s])
            for o in range(1, X):
                block = full.at[zz, at(y, Y - p, Y), at(x, X - o, X), 1 - core]
                index = (o - 1, p - 1, s)
                arrived(block.at[lower], dxy_ss.at[index], dxy_rs.at[index])
                arrived(block.at[upper], dyx_ss.at[index], dyx_rs.at[index])
    for copy in sends:
        copy.wait_send()


def local(dims, grads, master, m_old, v_old, old_bounds):
    Z, Y, X = dims
    count = Z * Y * X * 2
    width = master.shape[0]
    rows = width // LANES
    half = rows // 2
    dma = pltpu.SemaphoreType.DMA
    two = lambda *shape: [dma(shape), dma(shape)]
    vmem = pltpu.VMEM
    outside = pl.BlockSpec(memory_space=pltpu.HBM)
    inside = pl.BlockSpec(memory_space=pltpu.VMEM)
    scratch = [
        vmem((X, Z, Y, half, LANES), F32), vmem((Y, Z, X, half, LANES), F32),
        vmem((X, Z, Y, half, LANES), F32), vmem((Y, Z, X, half, LANES), F32),
        vmem((X - 1, Z, Y, half, LANES), BF16), vmem((Y - 1, Z, X, half, LANES), BF16),
        vmem((X - 1, Z, Y, half, LANES), BF16), vmem((Y - 1, Z, X, half, LANES), BF16),
        vmem((Y - 1, Z, half, LANES), BF16), vmem((X - 1, Z, half, LANES), BF16),
        vmem((Y - 1, Z, half, LANES), BF16), vmem((X - 1, Z, half, LANES), BF16),
        vmem((Z, half, LANES), F32), vmem((Z, half, LANES), F32),
        vmem((Z - 1, rows, LANES), BF16), vmem((Z - 1, rows, LANES), BF16),
        vmem((rows, LANES), F32),
        vmem((2, 3 * rows + 8, LANES), F32), vmem((2, rows, LANES), F32),
        vmem((2, 2, half, LANES), BF16), vmem((2, 2, half, LANES), BF16),
        vmem((2, rows, LANES), F32), vmem((rows, LANES), F32),
        vmem((1, LANES), F32), vmem((count, 1, LANES), F32),
        dma((3,)), dma((X, Z)), dma((Y, Z)),
        *two(X, Z), *two(Y, Z),
        *two(X - 1, Z), *two(Y - 1, Z), *two(Y - 1, Z), *two(X - 1, Z), *two(Z - 1),
        *two(2), *two(count),
        *two(Z - 1), *two(X - 1, Z), *two(Y - 1, Z), *two(X - 1, Y - 1, Z), *two(X - 1, Y - 1, Z),
        *two(Z), *two(X - 1, Z), *two(Y - 1, Z), *two(X - 1, Y - 1, Z), *two(X - 1, Y - 1, Z),
    ]
    results = 12 * width + 2 * count * width
    flat = jax.ShapeDtypeStruct((rows, LANES), F32)
    master_new, m_new, v_new, full = pl.pallas_call(
        functools.partial(kernel, dims),
        out_shape=(pltpu.VMEM((rows, LANES), F32),) * 3 + (pltpu.VMEM((Z, Y, X, 2, rows, LANES), BF16),),
        in_specs=[outside] * 4 + [pl.BlockSpec(memory_space=pltpu.SMEM)],
        out_specs=(inside,) * 4,
        scratch_shapes=scratch,
        compiler_params=pltpu.CompilerParams(
            collective_id=0, has_side_effects=True, vmem_limit_bytes=VMEM_BYTES - results),
    )(
        grads.reshape(Z, Y, X, 2, rows, LANES),
        master.reshape(rows, LANES),
        m_old.reshape(2 * rows, LANES),
        v_old.reshape(2 * rows, LANES),
        old_bounds,
    )

    def publish(*refs):
        ins, outs, sem = refs[:4], refs[4:8], refs[8]
        copies = [pltpu.make_async_copy(i, o, sem.at[k]) for k, (i, o) in enumerate(zip(ins, outs))]
        for c in copies:
            c.start()
        for c in copies:
            c.wait()

    master_new, m_new, v_new, full = [pltpu.with_memory_space_constraint(t, pltpu.VMEM) for t in (master_new, m_new, v_new, full)]
    master_new, m_new, v_new, full = pl.pallas_call(
        publish,
        out_shape=(flat, flat, flat, jax.ShapeDtypeStruct((Z, Y, X, 2, rows, LANES), BF16)),
        in_specs=[inside] * 4,
        out_specs=(outside,) * 4,
        scratch_shapes=[dma((4,))],
        compiler_params=pltpu.CompilerParams(vmem_limit_bytes=1024 * 1024),
    )(master_new, m_new, v_new, full)
    return (master_new.reshape(width), m_new.reshape(width), v_new.reshape(width), full.reshape(count * width))


def solution(mesh):
    dims = grid_of(mesh.shape["dp"])
    return jax.shard_map(
        functools.partial(local, dims),
        mesh=mesh,
        in_specs=(P("dp", None), P("dp"), P("dp", None), P("dp", None), P()),
        out_specs=(P("dp"), P("dp"), P("dp"), P()),
        check_vma=False,
    )
```

```python
import functools

import jax
import jax.numpy as jnp
from jax import lax
from jax.experimental import pallas as pl
from jax.experimental.pallas import tpu as pltpu
from jax.sharding import PartitionSpec as P

MESH = pl.DeviceIdType.MESH
LANES = 128
AHEAD = 2
VMEM_BYTES = 127 * 512 * 1024
F32 = jnp.float32
BF16 = jnp.bfloat16


def grid_of(count):
    sizes, chips, turn = [1, 1, 1], count // 2, 0
    while chips > 1:
        sizes[turn % 3] *= 2
        chips //= 2
        turn += 1
    return tuple(sizes)


def kernel(
    dims, grads, master, m_old, v_old, bounds,
    master_out, m_out, v_out, full,
    own_a, own_b, mate_a, mate_b,
    send_a1, send_b1, recv_a1, recv_b1,
    send_a2, send_b2, recv_a2, recv_b2, keep_a, keep_b,
    send_z, recv_z, gradient,
    spans, here, edge_out, edge_in, prev, weights, norm_out, norm_in,
    load_sem, own_sem_a, own_sem_b,
    mate_ss_a, mate_rs_a, mate_ss_b, mate_rs_b,
    ss_a1, rs_a1, ss_b1, rs_b1, ss_a2, rs_a2, ss_b2, rs_b2, ss_z, rs_z,
    edge_ss, edge_rs, norm_ss, norm_rs,
    gz_ss, gz_rs, gx_ss, gx_rs, gy_ss, gy_rs, gxy_ss, gxy_rs, gyx_ss, gyx_rs,
    d_ss, d_rs, dx_ss, dx_rs, dy_ss, dy_rs, dxy_ss, dxy_rs, dyx_ss, dyx_rs,
):
    Z, Y, X = dims
    count = Z * Y * X * 2
    rows = master.shape[0]
    half = rows // 2
    me = lax.axis_index("dp")
    core = me % 2
    x = (me // 2) % X
    y = (me // (2 * X)) % Y
    z = me // (2 * X * Y)

    def device(zz, yy, xx, cc):
        return ((zz * Y + yy) * X + xx) * 2 + cc

    mate = device(z, y, x, 1 - core)

    def at(coord, step, size):
        return (coord + step) % size

    sends = []

    def send(src, dst, ss, rs, target):
        copy = pltpu.make_async_remote_copy(
            src_ref=src, dst_ref=dst, send_sem=ss, recv_sem=rs,
            device_id=(target,), device_id_type=MESH)
        copy.start()
        sends.append(copy)

    def arrived(dst, ss, rs):
        pltpu.make_async_remote_copy(
            src_ref=dst, dst_ref=dst, send_sem=ss, recv_sem=rs,
            device_id=(mate,), device_id_type=MESH).wait_recv()

    barrier = pltpu.get_barrier_semaphore()

    peers = [(me + 1) % count, (me + count - 1) % count]
    peers += [device(at(z, s, Z), y, x, core) for s in range(1, Z)]
    peers += [device(z, at(y, o, Y), x, core) for o in range(1, Y)]
    peers += [device(z, y, at(x, o, X), core) for o in range(1, X)]
    for peer in peers:
        pl.semaphore_signal(barrier, inc=1, device_id=(peer,), device_id_type=MESH)

    pad = rows + 8
    load_m = pltpu.make_async_copy(m_old, spans.at[0, pl.ds(pad, 2 * rows)], load_sem.at[0])
    load_v = pltpu.make_async_copy(v_old, spans.at[1, pl.ds(pad, 2 * rows)], load_sem.at[1])
    load_w = pltpu.make_async_copy(master, weights, load_sem.at[2])
    load_m.start()
    load_v.start()
    order = [s for s in sorted(range(1, Z), key=lambda s: abs(s - Z / 2))] + [0]
    first, second = slice(0, half), slice(half, rows)
    loads_a, loads_b = {}, {}
    for s in order:
        for o in list(range(1, X)) + [0]:
            loads_a[o, s] = pltpu.make_async_copy(
                grads.at[at(z, s, Z), :, at(x, o, X), core, pl.ds(0, half)],
                own_a.at[o, s], own_sem_a.at[o, s])
            loads_a[o, s].start()
        for o in list(range(1, Y)) + [0]:
            loads_b[o, s] = pltpu.make_async_copy(
                grads.at[at(z, s, Z), at(y, o, Y), :, core, pl.ds(half, half)],
                own_b.at[o, s], own_sem_b.at[o, s])
            loads_b[o, s].start()
    load_w.start()

    here_bound = bounds[me] - me * (rows * LANES)
    next_bound = bounds[me + 1] - me * (rows * LANES)
    shift = jnp.clip(here_bound + half * LANES, 0, rows * LANES)
    lift, turn = shift // LANES, shift % LANES
    spans[:, pl.ds(0, pad)] = jnp.zeros((2, pad, LANES), F32)
    load_m.wait()
    load_v.wait()
    tile = 32
    lane = lax.broadcasted_iota(jnp.int32, (tile, LANES), 1)

    def aligned(which, row):
        base = pad + row - lift
        now = pltpu.roll(spans[which, pl.ds(base, tile)], turn, 1)
        before = pltpu.roll(spans[which, pl.ds(base - 1, tile)], turn, 1)
        return jnp.where(lane >= turn, now, before)

    for which in range(2):
        @pl.loop(0, half // tile)
        def _(i, which=which):
            row = pl.multiple_of(i * tile, tile)
            edge_out[0, which, pl.ds(row, tile)] = aligned(which, row).astype(BF16)
            edge_out[1, which, pl.ds(row, tile)] = aligned(which, row + 3 * half).astype(BF16)
            here[which, pl.ds(row, tile)] = aligned(which, row + half)
            here[which, pl.ds(row + half, tile)] = aligned(which, row + 2 * half)

    pl.semaphore_wait(barrier, len(peers))

    def swap_a(o, s):
        send(grads.at[at(z, s, Z), :, at(x, o, X), 1 - core, pl.ds(0, half)],
             mate_a.at[o, s], mate_ss_a.at[o, s], mate_rs_a.at[o, s], mate)

    def swap_b(o, s):
        send(grads.at[at(z, s, Z), at(y, o, Y), :, 1 - core, pl.ds(half, half)],
             mate_b.at[o, s], mate_ss_b.at[o, s], mate_rs_b.at[o, s], mate)

    for s in order:
        for o in range(1, X):
            swap_a(o, s)
        for o in range(1, Y):
            swap_b(o, s)
    for s in order:
        swap_a(0, s)
        swap_b(0, s)

    def chip_ready_a(o, s):
        loads_a[o, s].wait()
        arrived(mate_a.at[o, s], mate_ss_a.at[o, s], mate_rs_a.at[o, s])

    def chip_ready_b(o, s):
        loads_b[o, s].wait()
        arrived(mate_b.at[o, s], mate_ss_b.at[o, s], mate_rs_b.at[o, s])

    def exchange_one(s):
        for o in range(1, X):
            chip_ready_a(o, s)
            for j in range(Y):
                send_a1[o - 1, s, j] = (own_a[o, s, j] + mate_a[o, s, j]).astype(BF16)
            send(send_a1.at[o - 1, s], recv_a1.at[o - 1, s], ss_a1.at[o - 1, s], rs_a1.at[o - 1, s],
                 device(z, y, at(x, o, X), core))
        for o in range(1, Y):
            chip_ready_b(o, s)
            for j in range(X):
                send_b1[o - 1, s, j] = (own_b[o, s, j] + mate_b[o, s, j]).astype(BF16)
            send(send_b1.at[o - 1, s], recv_b1.at[o - 1, s], ss_b1.at[o - 1, s], rs_b1.at[o - 1, s],
                 device(z, at(y, o, Y), x, core))

    def exchange_two(s):
        chip_ready_a(0, s)
        for o in range(1, X):
            arrived(recv_a1.at[o - 1, s], ss_a1.at[o - 1, s], rs_a1.at[o - 1, s])

        def sum_a(j):
            value = own_a[0, s, j] + mate_a[0, s, j]
            for o in range(1, X):
                value = value + recv_a1[o - 1, s, j].astype(F32)
            return value

        for o in range(1, Y):
            send_a2[o - 1, s] = sum_a(at(y, o, Y)).astype(BF16)
            send(send_a2.at[o - 1, s], recv_a2.at[o - 1, s], ss_a2.at[o - 1, s], rs_a2.at[o - 1, s],
                 device(z, at(y, o, Y), x, core))
        keep_a[s] = sum_a(y)
        chip_ready_b(0, s)
        for o in range(1, Y):
            arrived(recv_b1.at[o - 1, s], ss_b1.at[o - 1, s], rs_b1.at[o - 1, s])

        def sum_b(j):
            value = own_b[0, s, j] + mate_b[0, s, j]
            for o in range(1, Y):
                value = value + recv_b1[o - 1, s, j].astype(F32)
            return value

        for o in range(1, X):
            send_b2[o - 1, s] = sum_b(at(x, o, X)).astype(BF16)
            send(send_b2.at[o - 1, s], recv_b2.at[o - 1, s], ss_b2.at[o - 1, s], rs_b2.at[o - 1, s],
                 device(z, y, at(x, o, X), core))
        keep_b[s] = sum_b(x)

    def exchange_three(s):
        for o in range(1, Y):
            arrived(recv_a2.at[o - 1, s], ss_a2.at[o - 1, s], rs_a2.at[o - 1, s])
        value_a = keep_a[s]
        for o in range(1, Y):
            value_a = value_a + recv_a2[o - 1, s].astype(F32)
        for o in range(1, X):
            arrived(recv_b2.at[o - 1, s], ss_b2.at[o - 1, s], rs_b2.at[o - 1, s])
        value_b = keep_b[s]
        for o in range(1, X):
            value_b = value_b + recv_b2[o - 1, s].astype(F32)
        if s == 0:
            gradient[pl.ds(0, half)] = value_a
            gradient[pl.ds(half, half)] = value_b
        else:
            send_z[s - 1, pl.ds(0, half)] = value_a.astype(BF16)
            send_z[s - 1, pl.ds(half, half)] = value_b.astype(BF16)
            send(send_z.at[s - 1], recv_z.at[s - 1], ss_z.at[s - 1], rs_z.at[s - 1],
                 device(at(z, s, Z), y, x, core))

    for s in order[:AHEAD]:
        exchange_one(s)
    send(edge_out.at[0], edge_in.at[0], edge_ss.at[0], edge_rs.at[0], (me + count - 1) % count)
    send(edge_out.at[1], edge_in.at[1], edge_ss.at[1], edge_rs.at[1], (me + 1) % count)
    for i in range(Z + 1):
        if i < Z:
            exchange_two(order[i])
        if AHEAD + i < Z:
            exchange_one(order[AHEAD + i])
        if i > 0:
            exchange_three(order[i - 1])
    for s in order[:-1]:
        arrived(recv_z.at[s - 1], ss_z.at[s - 1], rs_z.at[s - 1])

    squares = jnp.zeros((8, LANES), F32)
    for i in range(rows // tile):
        part = gradient[pl.ds(i * tile, tile)]
        for s in order[:-1]:
            part = part + recv_z[s - 1, pl.ds(i * tile, tile)].astype(F32)
        gradient[pl.ds(i * tile, tile)] = part
        squares = squares + jnp.sum((part * part).reshape(tile // 8, 8, LANES), axis=0)
    mine = jnp.sum(squares, axis=0, keepdims=True)
    norm_out[...] = mine
    norm_in[me] = mine

    @pl.loop(1, count)
    def _(step):
        pltpu.make_async_remote_copy(
            src_ref=norm_out, dst_ref=norm_in.at[me], send_sem=norm_ss.at[step], recv_sem=norm_rs.at[me],
            device_id=((me + step) % count,), device_id_type=MESH).start()

    for e in range(2):
        arrived(edge_in.at[e], edge_ss.at[e], edge_rs.at[e])
    place = lax.broadcasted_iota(jnp.int32, (tile, LANES), 0) * LANES + lane

    @pl.loop(0, half // tile)
    def _(i):
        row = pl.multiple_of(i * tile, tile)
        low = row * LANES + place
        high = low + half * LANES
        for which in range(2):
            prev[which, pl.ds(row, tile)] = jnp.where(
                low < here_bound, edge_in[1, which, pl.ds(row, tile)].astype(F32),
                here[which, pl.ds(row, tile)])
            prev[which, pl.ds(row + half, tile)] = jnp.where(
                high >= next_bound, edge_in[0, which, pl.ds(row, tile)].astype(F32),
                here[which, pl.ds(row + half, tile)])

    load_w.wait()

    @pl.loop(1, count)
    def _(step):
        other = (me + step) % count
        pltpu.make_async_remote_copy(
            src_ref=norm_out, dst_ref=norm_in.at[other], send_sem=norm_ss.at[step], recv_sem=norm_rs.at[other],
            device_id=(other,), device_id_type=MESH).wait()

    total = jnp.sum(jnp.sum(norm_in[...], axis=0), axis=1, keepdims=True)
    size = jnp.float32(count * rows * LANES)
    clip = jnp.minimum(1.0, jnp.sqrt(size) / (jnp.sqrt(total) + 1e-06))

    for i in range(rows // tile):
        part = pl.ds(i * tile, tile)
        clipped = clip * gradient[part]
        m_new = 0.5 * prev[0, part] + 0.5 * clipped
        v_new = 0.95 * prev[1, part] + 0.05 * clipped * clipped
        direction = m_new / (1.0 - 0.5**20) / (jnp.sqrt(v_new / (1.0 - 0.95**20)) + 1e-08)
        weight = weights[part]
        weight = weight - 0.05 * (direction + 0.1 * weight)
        full[z, y, x, core, part] = weight.astype(BF16)
        master_out[part] = weight
        m_out[part] = m_new
        v_out[part] = v_new

    lower, upper = pl.ds(0, half), pl.ds(half, half)

    def spread(s):
        zz = at(z, Z - s, Z)
        block = full.at[zz, y, x, core]
        if s > 0:
            arrived(block, gz_ss.at[s - 1], gz_rs.at[s - 1])
        for o in range(1, X):
            send(block, block, gx_ss.at[o - 1, s], gx_rs.at[o - 1, s], device(z, y, at(x, o, X), core))
        for o in range(1, Y):
            send(block, block, gy_ss.at[o - 1, s], gy_rs.at[o - 1, s], device(z, at(y, o, Y), x, core))
        send(block, block, d_ss.at[s], d_rs.at[s], mate)

    def turn_corner(s):
        zz = at(z, Z - s, Z)
        for o in range(1, X):
            block = full.at[zz, y, at(x, X - o, X), core]
            arrived(block, gx_ss.at[o - 1, s], gx_rs.at[o - 1, s])
            for p in range(1, Y):
                send(block.at[lower], block.at[lower], gxy_ss.at[o - 1, p - 1, s], gxy_rs.at[o - 1, p - 1, s],
                     device(z, at(y, p, Y), x, core))
            send(block, block, dx_ss.at[o - 1, s], dx_rs.at[o - 1, s], mate)
        for p in range(1, Y):
            block = full.at[zz, at(y, Y - p, Y), x, core]
            arrived(block, gy_ss.at[p - 1, s], gy_rs.at[p - 1, s])
            for o in range(1, X):
                send(block.at[upper], block.at[upper], gyx_ss.at[o - 1, p - 1, s], gyx_rs.at[o - 1, p - 1, s],
                     device(z, y, at(x, o, X), core))
            send(block, block, dy_ss.at[p - 1, s], dy_rs.at[p - 1, s], mate)

    def finish(s):
        zz = at(z, Z - s, Z)
        for o in range(1, X):
            for p in range(1, Y):
                block = full.at[zz, at(y, Y - p, Y), at(x, X - o, X), core]
                index = (o - 1, p - 1, s)
                arrived(block.at[lower], gxy_ss.at[index], gxy_rs.at[index])
                send(block.at[lower], block.at[lower], dxy_ss.at[index], dxy_rs.at[index], mate)
                arrived(block.at[upper], gyx_ss.at[index], gyx_rs.at[index])
                send(block.at[upper], block.at[upper], dyx_ss.at[index], dyx_rs.at[index], mate)

    mine = full.at[z, y, x, core]
    ring = [0] + sorted(range(1, Z), key=lambda s: -abs(s - Z / 2))
    for s in ring[1:]:
        send(mine, mine, gz_ss.at[s - 1], gz_rs.at[s - 1], device(at(z, s, Z), y, x, core))
    for i in range(Z + 2):
        if i < Z:
            spread(ring[i])
        if 0 <= i - 1 < Z:
            turn_corner(ring[i - 1])
        if 0 <= i - 2 < Z:
            finish(ring[i - 2])
    for s in range(Z):
        zz = at(z, Z - s, Z)
        arrived(full.at[zz, y, x, 1 - core], d_ss.at[s], d_rs.at[s])
        for o in range(1, X):
            arrived(full.at[zz, y, at(x, X - o, X), 1 - core], dx_ss.at[o - 1, s], dx_rs.at[o - 1, s])
        for p in range(1, Y):
            arrived(full.at[zz, at(y, Y - p, Y), x, 1 - core], dy_ss.at[p - 1, s], dy_rs.at[p - 1, s])
            for o in range(1, X):
                block = full.at[zz, at(y, Y - p, Y), at(x, X - o, X), 1 - core]
                index = (o - 1, p - 1, s)
                arrived(block.at[lower], dxy_ss.at[index], dxy_rs.at[index])
                arrived(block.at[upper], dyx_ss.at[index], dyx_rs.at[index])
    for copy in sends:
        copy.wait_send()


def local(dims, grads, master, m_old, v_old, old_bounds):
    Z, Y, X = dims
    count = Z * Y * X * 2
    width = master.shape[0]
    rows = width // LANES
    half = rows // 2
    dma = pltpu.SemaphoreType.DMA
    two = lambda *shape: [dma(shape), dma(shape)]
    vmem = pltpu.VMEM
    outside = pl.BlockSpec(memory_space=pltpu.HBM)
    inside = pl.BlockSpec(memory_space=pltpu.VMEM)
    scratch = [
        vmem((X, Z, Y, half, LANES), F32), vmem((Y, Z, X, half, LANES), F32),
        vmem((X, Z, Y, half, LANES), F32), vmem((Y, Z, X, half, LANES), F32),
        vmem((X - 1, Z, Y, half, LANES), BF16), vmem((Y - 1, Z, X, half, LANES), BF16),
        vmem((X - 1, Z, Y, half, LANES), BF16), vmem((Y - 1, Z, X, half, LANES), BF16),
        vmem((Y - 1, Z, half, LANES), BF16), vmem((X - 1, Z, half, LANES), BF16),
        vmem((Y - 1, Z, half, LANES), BF16), vmem((X - 1, Z, half, LANES), BF16),
        vmem((Z, half, LANES), F32), vmem((Z, half, LANES), F32),
        vmem((Z - 1, rows, LANES), BF16), vmem((Z - 1, rows, LANES), BF16),
        vmem((rows, LANES), F32),
        vmem((2, 3 * rows + 8, LANES), F32), vmem((2, rows, LANES), F32),
        vmem((2, 2, half, LANES), BF16), vmem((2, 2, half, LANES), BF16),
        vmem((2, rows, LANES), F32), vmem((rows, LANES), F32),
        vmem((1, LANES), F32), vmem((count, 1, LANES), F32),
        dma((3,)), dma((X, Z)), dma((Y, Z)),
        *two(X, Z), *two(Y, Z),
        *two(X - 1, Z), *two(Y - 1, Z), *two(Y - 1, Z), *two(X - 1, Z), *two(Z - 1),
        *two(2), *two(count),
        *two(Z - 1), *two(X - 1, Z), *two(Y - 1, Z), *two(X - 1, Y - 1, Z), *two(X - 1, Y - 1, Z),
        *two(Z), *two(X - 1, Z), *two(Y - 1, Z), *two(X - 1, Y - 1, Z), *two(X - 1, Y - 1, Z),
    ]
    results = 12 * width + 2 * count * width
    flat = jax.ShapeDtypeStruct((rows, LANES), F32)
    master_new, m_new, v_new, full = pl.pallas_call(
        functools.partial(kernel, dims),
        out_shape=(pltpu.VMEM((rows, LANES), F32),) * 3 + (pltpu.VMEM((Z, Y, X, 2, rows, LANES), BF16),),
        in_specs=[outside] * 4 + [pl.BlockSpec(memory_space=pltpu.SMEM)],
        out_specs=(inside,) * 4,
        scratch_shapes=scratch,
        compiler_params=pltpu.CompilerParams(
            collective_id=0, has_side_effects=True, vmem_limit_bytes=VMEM_BYTES - results),
    )(
        grads.reshape(Z, Y, X, 2, rows, LANES),
        master.reshape(rows, LANES),
        m_old.reshape(2 * rows, LANES),
        v_old.reshape(2 * rows, LANES),
        old_bounds,
    )

    def publish(*refs):
        ins, outs, sem = refs[:4], refs[4:8], refs[8]
        copies = [pltpu.make_async_copy(i, o, sem.at[k]) for k, (i, o) in enumerate(zip(ins, outs))]
        for c in copies:
            c.start()
        for c in copies:
            c.wait()

    master_new, m_new, v_new, full = [pltpu.with_memory_space_constraint(t, pltpu.VMEM) for t in (master_new, m_new, v_new, full)]
    master_new, m_new, v_new, full = pl.pallas_call(
        publish,
        out_shape=(flat, flat, flat, jax.ShapeDtypeStruct((Z, Y, X, 2, rows, LANES), BF16)),
        in_specs=[inside] * 4,
        out_specs=(outside,) * 4,
        scratch_shapes=[dma((4,))],
        compiler_params=pltpu.CompilerParams(vmem_limit_bytes=1024 * 1024),
    )(master_new, m_new, v_new, full)
    return (master_new.reshape(width), m_new.reshape(width), v_new.reshape(width), full.reshape(count * width))


def solution(mesh):
    dims = grid_of(mesh.shape["dp"])
    return jax.shard_map(
        functools.partial(local, dims),
        mesh=mesh,
        in_specs=(P("dp", None), P("dp"), P("dp", None), P("dp", None), P()),
        out_specs=(P("dp"), P("dp"), P("dp"), P()),
        check_vma=False,
    )
```

```python
import functools

import jax
import jax.numpy as jnp
from jax import lax
from jax.experimental import pallas as pl
from jax.experimental.pallas import tpu as pltpu
from jax.sharding import PartitionSpec as P

MESH = pl.DeviceIdType.MESH
LANES = 128
AHEAD = 2
LAG = 3
VMEM_BYTES = 127 * 512 * 1024
F32 = jnp.float32
BF16 = jnp.bfloat16


def grid_of(count):
    sizes, chips, turn = [1, 1, 1], count // 2, 0
    while chips > 1:
        sizes[turn % 3] *= 2
        chips //= 2
        turn += 1
    return tuple(sizes)


def kernel(
    dims, grads, master, m_old, v_old, bounds,
    master_out, m_out, v_out, full,
    own_a, own_b, mate_a, mate_b, out_a, out_b,
    send_a1, send_b1, recv_a1, recv_b1,
    send_a2, send_b2, recv_a2, recv_b2, keep_a, keep_b,
    send_z, recv_z, gradient,
    spans, here, edge_out, edge_in, prev, weights, norm_out, norm_in,
    load_sem, own_sem_a, own_sem_b, out_sem_a, out_sem_b,
    mate_ss_a, mate_rs_a, mate_ss_b, mate_rs_b,
    ss_a1, rs_a1, ss_b1, rs_b1, ss_a2, rs_a2, ss_b2, rs_b2, ss_z, rs_z,
    edge_ss, edge_rs, norm_ss, norm_rs,
    gz_ss, gz_rs, gx_ss, gx_rs, gy_ss, gy_rs, hx_ss, hx_rs, hy_ss, hy_rs, gxy_ss, gxy_rs, gyx_ss, gyx_rs,
    d_ss, d_rs, dx_ss, dx_rs, dy_ss, dy_rs, dxy_ss, dxy_rs, dyx_ss, dyx_rs,
):
    Z, Y, X = dims
    count = Z * Y * X * 2
    rows = master.shape[0]
    half = rows // 2
    me = lax.axis_index("dp")
    core = me % 2
    x = (me // 2) % X
    y = (me // (2 * X)) % Y
    z = me // (2 * X * Y)

    def device(zz, yy, xx, cc):
        return ((zz * Y + yy) * X + xx) * 2 + cc

    mate = device(z, y, x, 1 - core)

    def at(coord, step, size):
        return (coord + step) % size

    sends = []

    def send(src, dst, ss, rs, target):
        copy = pltpu.make_async_remote_copy(
            src_ref=src, dst_ref=dst, send_sem=ss, recv_sem=rs,
            device_id=(target,), device_id_type=MESH)
        copy.start()
        sends.append(copy)

    def arrived(dst, ss, rs):
        pltpu.make_async_remote_copy(
            src_ref=dst, dst_ref=dst, send_sem=ss, recv_sem=rs,
            device_id=(mate,), device_id_type=MESH).wait_recv()

    barrier = pltpu.get_barrier_semaphore()

    peers = [(me + 1) % count, (me + count - 1) % count]
    peers += [device(at(z, s, Z), y, x, core) for s in range(1, Z)]
    peers += [device(z, at(y, o, Y), x, core) for o in range(1, Y)]
    peers += [device(z, y, at(x, o, X), core) for o in range(1, X)]
    for peer in peers:
        pl.semaphore_signal(barrier, inc=1, device_id=(peer,), device_id_type=MESH)

    pad = rows + 8
    load_m = pltpu.make_async_copy(m_old, spans.at[0, pl.ds(pad, 2 * rows)], load_sem.at[0])
    load_v = pltpu.make_async_copy(v_old, spans.at[1, pl.ds(pad, 2 * rows)], load_sem.at[1])
    load_w = pltpu.make_async_copy(master, weights, load_sem.at[2])
    load_m.start()
    load_v.start()
    order = [s for s in sorted(range(1, Z), key=lambda s: abs(s - Z / 2))] + [0]
    loads_a, loads_b, stage_a, stage_b = {}, {}, {}, {}
    for s in order:
        for o in range(1, X):
            stage_a[o, s] = pltpu.make_async_copy(
                grads.at[at(z, s, Z), :, at(x, o, X), 1 - core, pl.ds(0, half)],
                out_a.at[o - 1, s], out_sem_a.at[o - 1, s])
            stage_a[o, s].start()
        for o in range(1, Y):
            stage_b[o, s] = pltpu.make_async_copy(
                grads.at[at(z, s, Z), at(y, o, Y), :, 1 - core, pl.ds(half, half)],
                out_b.at[o - 1, s], out_sem_b.at[o - 1, s])
            stage_b[o, s].start()
    for s in order:
        for o in list(range(1, X)) + [0]:
            loads_a[o, s] = pltpu.make_async_copy(
                grads.at[at(z, s, Z), :, at(x, o, X), core, pl.ds(0, half)],
                own_a.at[o, s], own_sem_a.at[o, s])
            loads_a[o, s].start()
        for o in list(range(1, Y)) + [0]:
            loads_b[o, s] = pltpu.make_async_copy(
                grads.at[at(z, s, Z), at(y, o, Y), :, core, pl.ds(half, half)],
                own_b.at[o, s], own_sem_b.at[o, s])
            loads_b[o, s].start()
    load_w.start()

    here_bound = bounds[me] - me * (rows * LANES)
    next_bound = bounds[me + 1] - me * (rows * LANES)
    shift = jnp.clip(here_bound + half * LANES, 0, rows * LANES)
    lift, turn = shift // LANES, shift % LANES
    spans[:, pl.ds(0, pad)] = jnp.zeros((2, pad, LANES), F32)
    load_m.wait()
    load_v.wait()
    tile = 32
    lane = lax.broadcasted_iota(jnp.int32, (tile, LANES), 1)

    def aligned(which, row):
        base = pad + row - lift
        now = pltpu.roll(spans[which, pl.ds(base, tile)], turn, 1)
        before = pltpu.roll(spans[which, pl.ds(base - 1, tile)], turn, 1)
        return jnp.where(lane >= turn, now, before)

    for which in range(2):
        @pl.loop(0, half // tile)
        def _(i, which=which):
            row = pl.multiple_of(i * tile, tile)
            edge_out[0, which, pl.ds(row, tile)] = aligned(which, row).astype(BF16)
            edge_out[1, which, pl.ds(row, tile)] = aligned(which, row + 3 * half).astype(BF16)
            here[which, pl.ds(row, tile)] = aligned(which, row + half)
            here[which, pl.ds(row + half, tile)] = aligned(which, row + 2 * half)

    pl.semaphore_wait(barrier, len(peers))

    def swap_a(o, s):
        if o > 0:
            stage_a[o, s].wait()
        send(out_a.at[o - 1, s] if o > 0 else grads.at[at(z, s, Z), :, x, 1 - core, pl.ds(0, half)],
             mate_a.at[o, s], mate_ss_a.at[o, s], mate_rs_a.at[o, s], mate)

    def swap_b(o, s):
        if o > 0:
            stage_b[o, s].wait()
        send(out_b.at[o - 1, s] if o > 0 else grads.at[at(z, s, Z), y, :, 1 - core, pl.ds(half, half)],
             mate_b.at[o, s], mate_ss_b.at[o, s], mate_rs_b.at[o, s], mate)

    for s in order:
        for o in range(1, X):
            swap_a(o, s)
        for o in range(1, Y):
            swap_b(o, s)
    for s in order:
        swap_a(0, s)
        swap_b(0, s)

    def chip_ready_a(o, s):
        loads_a[o, s].wait()
        arrived(mate_a.at[o, s], mate_ss_a.at[o, s], mate_rs_a.at[o, s])

    def chip_ready_b(o, s):
        loads_b[o, s].wait()
        arrived(mate_b.at[o, s], mate_ss_b.at[o, s], mate_rs_b.at[o, s])

    def exchange_one(s):
        for o in range(1, X):
            chip_ready_a(o, s)
            for j in range(Y):
                send_a1[o - 1, s, j] = (own_a[o, s, j] + mate_a[o, s, j]).astype(BF16)
            send(send_a1.at[o - 1, s], recv_a1.at[o - 1, s], ss_a1.at[o - 1, s], rs_a1.at[o - 1, s],
                 device(z, y, at(x, o, X), core))
        for o in range(1, Y):
            chip_ready_b(o, s)
            for j in range(X):
                send_b1[o - 1, s, j] = (own_b[o, s, j] + mate_b[o, s, j]).astype(BF16)
            send(send_b1.at[o - 1, s], recv_b1.at[o - 1, s], ss_b1.at[o - 1, s], rs_b1.at[o - 1, s],
                 device(z, at(y, o, Y), x, core))

    def exchange_two(s):
        chip_ready_a(0, s)
        for o in range(1, X):
            arrived(recv_a1.at[o - 1, s], ss_a1.at[o - 1, s], rs_a1.at[o - 1, s])

        def sum_a(j):
            value = own_a[0, s, j] + mate_a[0, s, j]
            for o in range(1, X):
                value = value + recv_a1[o - 1, s, j].astype(F32)
            return value

        for o in range(1, Y):
            send_a2[o - 1, s] = sum_a(at(y, o, Y)).astype(BF16)
            send(send_a2.at[o - 1, s], recv_a2.at[o - 1, s], ss_a2.at[o - 1, s], rs_a2.at[o - 1, s],
                 device(z, at(y, o, Y), x, core))
        keep_a[s] = sum_a(y)
        chip_ready_b(0, s)
        for o in range(1, Y):
            arrived(recv_b1.at[o - 1, s], ss_b1.at[o - 1, s], rs_b1.at[o - 1, s])

        def sum_b(j):
            value = own_b[0, s, j] + mate_b[0, s, j]
            for o in range(1, Y):
                value = value + recv_b1[o - 1, s, j].astype(F32)
            return value

        for o in range(1, X):
            send_b2[o - 1, s] = sum_b(at(x, o, X)).astype(BF16)
            send(send_b2.at[o - 1, s], recv_b2.at[o - 1, s], ss_b2.at[o - 1, s], rs_b2.at[o - 1, s],
                 device(z, y, at(x, o, X), core))
        keep_b[s] = sum_b(x)

    def exchange_three(s):
        for o in range(1, Y):
            arrived(recv_a2.at[o - 1, s], ss_a2.at[o - 1, s], rs_a2.at[o - 1, s])
        value_a = keep_a[s]
        for o in range(1, Y):
            value_a = value_a + recv_a2[o - 1, s].astype(F32)
        for o in range(1, X):
            arrived(recv_b2.at[o - 1, s], ss_b2.at[o - 1, s], rs_b2.at[o - 1, s])
        value_b = keep_b[s]
        for o in range(1, X):
            value_b = value_b + recv_b2[o - 1, s].astype(F32)
        if s == 0:
            gradient[pl.ds(0, half)] = value_a
            gradient[pl.ds(half, half)] = value_b
        else:
            send_z[s - 1, pl.ds(0, half)] = value_a.astype(BF16)
            send_z[s - 1, pl.ds(half, half)] = value_b.astype(BF16)
            send(send_z.at[s - 1], recv_z.at[s - 1], ss_z.at[s - 1], rs_z.at[s - 1],
                 device(at(z, s, Z), y, x, core))

    for s in order[:AHEAD]:
        exchange_one(s)
    send(edge_out.at[0], edge_in.at[0], edge_ss.at[0], edge_rs.at[0], (me + count - 1) % count)
    send(edge_out.at[1], edge_in.at[1], edge_ss.at[1], edge_rs.at[1], (me + 1) % count)
    for i in range(Z + 1):
        if i < Z:
            exchange_two(order[i])
        if AHEAD + i < Z:
            exchange_one(order[AHEAD + i])
        if i > 0:
            exchange_three(order[i - 1])
    for s in order[:-1]:
        arrived(recv_z.at[s - 1], ss_z.at[s - 1], rs_z.at[s - 1])

    squares = jnp.zeros((8, LANES), F32)
    for i in range(rows // tile):
        part = gradient[pl.ds(i * tile, tile)]
        for s in order[:-1]:
            part = part + recv_z[s - 1, pl.ds(i * tile, tile)].astype(F32)
        gradient[pl.ds(i * tile, tile)] = part
        squares = squares + jnp.sum((part * part).reshape(tile // 8, 8, LANES), axis=0)
    mine = jnp.sum(squares, axis=0, keepdims=True)
    norm_out[...] = mine
    norm_in[me] = mine

    @pl.loop(1, count)
    def _(step):
        pltpu.make_async_remote_copy(
            src_ref=norm_out, dst_ref=norm_in.at[me], send_sem=norm_ss.at[step], recv_sem=norm_rs.at[me],
            device_id=((me + step) % count,), device_id_type=MESH).start()

    for e in range(2):
        arrived(edge_in.at[e], edge_ss.at[e], edge_rs.at[e])
    place = lax.broadcasted_iota(jnp.int32, (tile, LANES), 0) * LANES + lane

    @pl.loop(0, half // tile)
    def _(i):
        row = pl.multiple_of(i * tile, tile)
        low = row * LANES + place
        high = low + half * LANES
        for which in range(2):
            prev[which, pl.ds(row, tile)] = jnp.where(
                low < here_bound, edge_in[1, which, pl.ds(row, tile)].astype(F32),
                here[which, pl.ds(row, tile)])
            prev[which, pl.ds(row + half, tile)] = jnp.where(
                high >= next_bound, edge_in[0, which, pl.ds(row, tile)].astype(F32),
                here[which, pl.ds(row + half, tile)])

    load_w.wait()

    @pl.loop(1, count)
    def _(step):
        other = (me + step) % count
        pltpu.make_async_remote_copy(
            src_ref=norm_out, dst_ref=norm_in.at[other], send_sem=norm_ss.at[step], recv_sem=norm_rs.at[other],
            device_id=(other,), device_id_type=MESH).wait()

    total = jnp.sum(jnp.sum(norm_in[...], axis=0), axis=1, keepdims=True)
    size = jnp.float32(count * rows * LANES)
    clip = jnp.minimum(1.0, jnp.sqrt(size) / (jnp.sqrt(total) + 1e-06))

    for i in range(rows // tile):
        part = pl.ds(i * tile, tile)
        clipped = clip * gradient[part]
        m_new = 0.5 * prev[0, part] + 0.5 * clipped
        v_new = 0.95 * prev[1, part] + 0.05 * clipped * clipped
        direction = m_new / (1.0 - 0.5**20) / (jnp.sqrt(v_new / (1.0 - 0.95**20)) + 1e-08)
        weight = weights[part]
        weight = weight - 0.05 * (direction + 0.1 * weight)
        full[z, y, x, core, part] = weight.astype(BF16)
        master_out[part] = weight
        m_out[part] = m_new
        v_out[part] = v_new

    lower, upper = pl.ds(0, half), pl.ds(half, half)

    def spread(s):
        zz = at(z, Z - s, Z)
        block = full.at[zz, y, x, core]
        if s > 0:
            arrived(block, gz_ss.at[s - 1], gz_rs.at[s - 1])
        for o in range(1, X):
            send(block.at[lower], block.at[lower], gx_ss.at[o - 1, s], gx_rs.at[o - 1, s], device(z, y, at(x, o, X), core))
        for o in range(1, Y):
            send(block.at[upper], block.at[upper], gy_ss.at[o - 1, s], gy_rs.at[o - 1, s], device(z, at(y, o, Y), x, core))
        for o in range(1, X):
            send(block.at[upper], block.at[upper], hx_ss.at[o - 1, s], hx_rs.at[o - 1, s], device(z, y, at(x, o, X), core))
        for o in range(1, Y):
            send(block.at[lower], block.at[lower], hy_ss.at[o - 1, s], hy_rs.at[o - 1, s], device(z, at(y, o, Y), x, core))
        send(block, block, d_ss.at[s], d_rs.at[s], mate)

    def turn_corner(s):
        zz = at(z, Z - s, Z)
        for o in range(1, X):
            block = full.at[zz, y, at(x, X - o, X), core]
            arrived(block.at[lower], gx_ss.at[o - 1, s], gx_rs.at[o - 1, s])
            for p in range(1, Y):
                send(block.at[lower], block.at[lower], gxy_ss.at[o - 1, p - 1, s], gxy_rs.at[o - 1, p - 1, s],
                     device(z, at(y, p, Y), x, core))
        for p in range(1, Y):
            block = full.at[zz, at(y, Y - p, Y), x, core]
            arrived(block.at[upper], gy_ss.at[p - 1, s], gy_rs.at[p - 1, s])
            for o in range(1, X):
                send(block.at[upper], block.at[upper], gyx_ss.at[o - 1, p - 1, s], gyx_rs.at[o - 1, p - 1, s],
                     device(z, y, at(x, o, X), core))

    def finish(s):
        zz = at(z, Z - s, Z)
        for o in range(1, X):
            block = full.at[zz, y, at(x, X - o, X), core]
            arrived(block.at[upper], hx_ss.at[o - 1, s], hx_rs.at[o - 1, s])
            send(block, block, dx_ss.at[o - 1, s], dx_rs.at[o - 1, s], mate)
        for p in range(1, Y):
            block = full.at[zz, at(y, Y - p, Y), x, core]
            arrived(block.at[lower], hy_ss.at[p - 1, s], hy_rs.at[p - 1, s])
            send(block, block, dy_ss.at[p - 1, s], dy_rs.at[p - 1, s], mate)
        for o in range(1, X):
            for p in range(1, Y):
                block = full.at[zz, at(y, Y - p, Y), at(x, X - o, X), core]
                index = (o - 1, p - 1, s)
                arrived(block.at[lower], gxy_ss.at[index], gxy_rs.at[index])
                send(block.at[lower], block.at[lower], dxy_ss.at[index], dxy_rs.at[index], mate)
                arrived(block.at[upper], gyx_ss.at[index], gyx_rs.at[index])
                send(block.at[upper], block.at[upper], dyx_ss.at[index], dyx_rs.at[index], mate)

    mine = full.at[z, y, x, core]
    ring = [0] + sorted(range(1, Z), key=lambda s: -abs(s - Z / 2))
    for s in ring[1:]:
        send(mine, mine, gz_ss.at[s - 1], gz_rs.at[s - 1], device(at(z, s, Z), y, x, core))
    for i in range(Z + LAG):
        if i < Z:
            spread(ring[i])
        if 0 <= i - 1 < Z:
            turn_corner(ring[i - 1])
        if 0 <= i - LAG < Z:
            finish(ring[i - LAG])
    for s in range(Z):
        zz = at(z, Z - s, Z)
        arrived(full.at[zz, y, x, 1 - core], d_ss.at[s], d_rs.at[s])
        for o in range(1, X):
            arrived(full.at[zz, y, at(x, X - o, X), 1 - core], dx_ss.at[o - 1, s], dx_rs.at[o - 1, s])
        for p in range(1, Y):
            arrived(full.at[zz, at(y, Y - p, Y), x, 1 - core], dy_ss.at[p - 1, s], dy_rs.at[p - 1, s])
            for o in range(1, X):
                block = full.at[zz, at(y, Y - p, Y), at(x, X - o, X), 1 - core]
                index = (o - 1, p - 1, s)
                arrived(block.at[lower], dxy_ss.at[index], dxy_rs.at[index])
                arrived(block.at[upper], dyx_ss.at[index], dyx_rs.at[index])
    for copy in sends:
        copy.wait_send()


def local(dims, grads, master, m_old, v_old, old_bounds):
    Z, Y, X = dims
    count = Z * Y * X * 2
    width = master.shape[0]
    rows = width // LANES
    half = rows // 2
    dma = pltpu.SemaphoreType.DMA
    two = lambda *shape: [dma(shape), dma(shape)]
    vmem = pltpu.VMEM
    outside = pl.BlockSpec(memory_space=pltpu.HBM)
    inside = pl.BlockSpec(memory_space=pltpu.VMEM)
    scratch = [
        vmem((X, Z, Y, half, LANES), F32), vmem((Y, Z, X, half, LANES), F32),
        vmem((X, Z, Y, half, LANES), F32), vmem((Y, Z, X, half, LANES), F32),
        vmem((X - 1, Z, Y, half, LANES), F32), vmem((Y - 1, Z, X, half, LANES), F32),
        vmem((X - 1, Z, Y, half, LANES), BF16), vmem((Y - 1, Z, X, half, LANES), BF16),
        vmem((X - 1, Z, Y, half, LANES), BF16), vmem((Y - 1, Z, X, half, LANES), BF16),
        vmem((Y - 1, Z, half, LANES), BF16), vmem((X - 1, Z, half, LANES), BF16),
        vmem((Y - 1, Z, half, LANES), BF16), vmem((X - 1, Z, half, LANES), BF16),
        vmem((Z, half, LANES), F32), vmem((Z, half, LANES), F32),
        vmem((Z - 1, rows, LANES), BF16), vmem((Z - 1, rows, LANES), BF16),
        vmem((rows, LANES), F32),
        vmem((2, 3 * rows + 8, LANES), F32), vmem((2, rows, LANES), F32),
        vmem((2, 2, half, LANES), BF16), vmem((2, 2, half, LANES), BF16),
        vmem((2, rows, LANES), F32), vmem((rows, LANES), F32),
        vmem((1, LANES), F32), vmem((count, 1, LANES), F32),
        dma((3,)), dma((X, Z)), dma((Y, Z)), dma((X - 1, Z)), dma((Y - 1, Z)),
        *two(X, Z), *two(Y, Z),
        *two(X - 1, Z), *two(Y - 1, Z), *two(Y - 1, Z), *two(X - 1, Z), *two(Z - 1),
        *two(2), *two(count),
        *two(Z - 1), *two(X - 1, Z), *two(Y - 1, Z), *two(X - 1, Z), *two(Y - 1, Z),
        *two(X - 1, Y - 1, Z), *two(X - 1, Y - 1, Z),
        *two(Z), *two(X - 1, Z), *two(Y - 1, Z), *two(X - 1, Y - 1, Z), *two(X - 1, Y - 1, Z),
    ]
    results = 12 * width + 2 * count * width
    flat = jax.ShapeDtypeStruct((rows, LANES), F32)
    master_new, m_new, v_new, full = pl.pallas_call(
        functools.partial(kernel, dims),
        out_shape=(pltpu.VMEM((rows, LANES), F32),) * 3 + (pltpu.VMEM((Z, Y, X, 2, rows, LANES), BF16),),
        in_specs=[outside] * 4 + [pl.BlockSpec(memory_space=pltpu.SMEM)],
        out_specs=(inside,) * 4,
        scratch_shapes=scratch,
        compiler_params=pltpu.CompilerParams(
            collective_id=0, has_side_effects=True, vmem_limit_bytes=VMEM_BYTES - results),
    )(
        grads.reshape(Z, Y, X, 2, rows, LANES),
        master.reshape(rows, LANES),
        m_old.reshape(2 * rows, LANES),
        v_old.reshape(2 * rows, LANES),
        old_bounds,
    )

    def publish(*refs):
        ins, outs, sem = refs[:4], refs[4:8], refs[8]
        copies = [pltpu.make_async_copy(i, o, sem.at[k]) for k, (i, o) in enumerate(zip(ins, outs))]
        for c in copies:
            c.start()
        for c in copies:
            c.wait()

    master_new, m_new, v_new, full = [pltpu.with_memory_space_constraint(t, pltpu.VMEM) for t in (master_new, m_new, v_new, full)]
    master_new, m_new, v_new, full = pl.pallas_call(
        publish,
        out_shape=(flat, flat, flat, jax.ShapeDtypeStruct((Z, Y, X, 2, rows, LANES), BF16)),
        in_specs=[inside] * 4,
        out_specs=(outside,) * 4,
        scratch_shapes=[dma((4,))],
        compiler_params=pltpu.CompilerParams(vmem_limit_bytes=1024 * 1024),
    )(master_new, m_new, v_new, full)
    return (master_new.reshape(width), m_new.reshape(width), v_new.reshape(width), full.reshape(count * width))


def solution(mesh):
    dims = grid_of(mesh.shape["dp"])
    return jax.shard_map(
        functools.partial(local, dims),
        mesh=mesh,
        in_specs=(P("dp", None), P("dp"), P("dp", None), P("dp", None), P()),
        out_specs=(P("dp"), P("dp"), P("dp"), P()),
        check_vma=False,
    )
```
